32 devices in a mesh: dp: 8 (over z, y), mp: 4 (over x, core).
Axes of the slice: x: 2, y: 2, z: 4, core: 2. Of those that a mesh axis runs over, the one named last changes fastest.
Arguments:
- gradient: bfloat16 [8, 64, 14336], P('dp', None, 'mp'), may hold values from -6 to 6
- momentum: float32 [8, 64, 14336], P('dp', None, 'mp'), may hold values from -6 to 6
- weights: float32 [64, 14336], P(None, 'mp'), may hold values from -6 to 6
- positions: int32 [8, 1, 224, 32], P('dp', None, 'mp'), may hold values from 0 to 4095, as said below
Outputs:
- new_momentum: float32 [8, 64, 14336], P('dp', None, 'mp')
- new_weights: float32 [64, 14336], P(None, 'mp')
The draws below stay inside these ranges and needn't reach their ends.
Inputs may be any that keep to these rules, and one draw needn't show every extreme that they name: Within one span of one replica the 32 positions are all different.
All inputs are finite; a program needn't handle non-finite values.
Results may differ from the reference program's by a relative error of at most 0.0003.
Values sent between devices are 32-bit elements; how exact they have to be, the bound alone decides.
No kernel may reach another device: no remote copies, remote signals or barrier semaphores. Data moves between devices by JAX's collectives and lax.ppermute only.
A program may use at most 64 MiB of HBM per device.

```python
import jax
import jax.numpy as jnp
from jax import lax

FF = 14336
BANDS = 1
K = 32
REPLICAS = 8
COLCH = 224


def draw_positions(key, part):
    scores = jax.random.randint(key, (REPLICAS, BANDS, FF // 64, 4096), 0, 262144, dtype=jnp.int32)
    scores = scores * 4096 + jnp.arange(4096, dtype=jnp.int32)
    chosen = jax.lax.top_k(scores, K)[1]
    return chosen.astype(jnp.int32)


def levels(own_key, dims, split, least, top_value):
    level, own = 1.0, jax.random.fold_in(own_key, 6)
    for dim, blocks in split:
        heights = jnp.exp(jax.random.uniform(jax.random.fold_in(own, dim), (blocks,), jnp.float32, least / len(split), top_value / len(split)))
        level = level * jnp.repeat(heights, dims[dim] // blocks).reshape([-1 if axis == dim else 1 for axis in range(len(dims))])
    return level


def normal_values(rng, extent, scale, most, shards=(), held_as=jnp.bfloat16):
    result = scale * jax.random.normal(rng, extent, jnp.float32)
    if shards:
        result = result * levels(rng, extent, shards, -0.22, 0.18)
    return jnp.clip(result, -most, most).astype(held_as)


def setup_inputs(seed: int = 0) -> dict:
    splits = jax.random.split(jax.random.key(seed), 5)
    gradient = normal_values(splits[0], (REPLICAS, 64 * BANDS, FF), 1.0, 6.0, ((0, 8), (2, 4)))
    momentum = normal_values(splits[1], (REPLICAS, 64 * BANDS, FF), 1.0, 6.0, ((0, 8), (2, 4)), jnp.float32)
    weights = normal_values(splits[2], (64 * BANDS, FF), 1.0, 6.0, ((1, 4),), jnp.float32)
    positions = draw_positions(jax.random.fold_in(splits[4], 71), 0)
    return {"gradient": gradient, "momentum": momentum, "weights": weights, "positions": positions}


def dct_table():
    column = jnp.arange(64, dtype=jnp.float32)
    freq = column[:, None]
    factor = jnp.where(freq == 0, jnp.sqrt(jnp.float32(1.0 / 64)), jnp.sqrt(jnp.float32(2.0 / 64)))
    return factor * jnp.cos(jnp.pi * (2.0 * column[None, :] + 1.0) * freq / 128.0)

def reference(gradient, momentum, weights, positions):
    table = dct_table()
    rows_all = 64 * BANDS
    band_index = jnp.arange(BANDS, dtype=jnp.int32)[:, None, None]
    span_index = jnp.arange(COLCH, dtype=jnp.int32)[None, :, None]

    def one_replica(carry, inputs):
        grad_one, mom_one, pos_one = inputs
        summed = 0.9 * mom_one + grad_one.astype(jnp.float32)
        blocks = summed.reshape(BANDS, 64, COLCH, 64)
        coefs = jnp.einsum('kr,brcs,ls->bckl', table, blocks, table, precision=lax.Precision.HIGHEST)
        flatten = coefs.reshape(BANDS, COLCH, 4096)
        picked = jnp.take_along_axis(flatten, pos_one, axis=2)
        own = jnp.zeros((BANDS, COLCH, 4096), jnp.float32).at[band_index, span_index, pos_one].add(picked)
        back = jnp.einsum('kr,bckl,ls->brcs', table, own.reshape(BANDS, COLCH, 64, 64), table, precision=lax.Precision.HIGHEST)
        return (carry + own, summed - back.reshape(rows_all, FF))
    start = jnp.zeros((BANDS, COLCH, 4096), jnp.float32)
    aggregate, new_momentum = lax.scan(one_replica, start, (gradient, momentum, positions))
    update = jnp.einsum('kr,bckl,ls->brcs', table, aggregate.reshape(BANDS, COLCH, 64, 64), table, precision=lax.Precision.HIGHEST)
    update = update.reshape(rows_all, FF)
    meansq = jnp.mean(update * update)
    new_weights = weights - update / jnp.sqrt(meansq + 1.0)
    return (new_momentum, new_weights)
```

```python
import functools

import jax
import jax.numpy as jnp
import numpy as np
from jax import lax
from jax.experimental import pallas as pl
from jax.experimental.pallas import tpu as pltpu
from jax.sharding import PartitionSpec as P

SPAN = 64
QUAD = 4
WIDE = SPAN * QUAD
F32 = jnp.float32
BF16 = jnp.bfloat16


def dct_table():
    column = np.arange(SPAN, dtype=np.float64)
    factor = np.where(column == 0, np.sqrt(1.0 / SPAN), np.sqrt(2.0 / SPAN))
    angle = np.pi * (2.0 * column[None, :] + 1.0) * column[:, None] / (2.0 * SPAN)
    return (factor[:, None] * np.cos(angle)).astype(np.float32)


def halves(table):
    high = table.astype(BF16)
    return high, (table - high.astype(np.float32)).astype(BF16)


def row_operand(table):
    high, low = halves(table)
    return np.concatenate([high, high, low], axis=1)


def lane_operand(table):
    return halves(np.kron(np.eye(QUAD, dtype=np.float32), table))


def split(value):
    high = value.astype(BF16)
    return high, (value - high.astype(F32)).astype(BF16)


def dot(left, right):
    return lax.dot_general(left, right, (((1,), (0,)), ((), ())), preferred_element_type=F32)


def dot_t(left, right):
    return lax.dot_general(left, right, (((1,), (1,)), ((), ())), preferred_element_type=F32)


def along_rows(operand, field):
    high, low = split(field)
    return dot(operand, jnp.concatenate([high, low, high], axis=0))


def along_lanes(field, high_table, low_table):
    high, low = split(field)
    return dot(high, high_table) + dot(low, high_table) + dot(high, low_table)


def lane_target(place):
    quarter = lax.broadcasted_iota(jnp.int32, place.shape, 1) // (128 // QUAD)
    return quarter * SPAN + place % SPAN


def hot(size, wanted):
    grid = lax.broadcasted_iota(jnp.int32, (size, wanted.shape[1]), 0)
    return grid == wanted


def pick_kernel(grad, mom, place, rows, high, low, message, coefs):
    groups = place.shape[0]
    message[...] = jnp.zeros_like(message)
    message[0, 16 : 16 + groups, :] = place[...].astype(F32)
    row_of = place[...] // SPAN
    lane_of = lane_target(place[...])
    for index in range(groups):
        lanes = slice(index * WIDE, (index + 1) * WIDE)
        summed = 0.9 * mom[0, :, lanes] + grad[0, :, lanes].astype(F32)
        along = along_rows(rows[...], summed)
        coef = along_lanes(along, high[...], low[...])
        coefs[:, lanes] = coef
        lane_hot = hot(WIDE, lane_of[index : index + 1]).astype(F32).astype(BF16)
        coef_high, coef_low = split(coef)
        columns = dot(coef_high, lane_hot) + dot(coef_low, lane_hot)
        chosen = jnp.where(hot(SPAN, row_of[index : index + 1]), columns, 0.0)
        message[0, index : index + 1, :] = jnp.sum(chosen, axis=0, keepdims=True)


def momentum_kernel(grad, mom, place, coefs, rows, high, low, out):
    groups = place.shape[0]
    row_of = place[...] // SPAN
    lane_of = lane_target(place[...])
    for index in range(groups):
        lanes = slice(index * WIDE, (index + 1) * WIDE)
        row_hot = hot(SPAN, row_of[index : index + 1]).astype(F32).astype(BF16)
        lane_hot = hot(WIDE, lane_of[index : index + 1]).astype(F32).astype(BF16)
        own = coefs[:, lanes] * dot_t(row_hot, lane_hot)
        across = along_lanes(own, high[...], low[...])
        back = along_rows(rows[...], across)
        summed = 0.9 * mom[0, :, lanes] + grad[0, :, lanes].astype(F32)
        out[0, :, lanes] = summed - back


def decode_group(index, order, lists, count):
    total = jnp.zeros((SPAN, WIDE), F32)
    for step in range(count):
        which = step ^ order
        value = lists[which, index : index + 1, :]
        place = lists[which, 16 + index : 17 + index, :].astype(jnp.int32)
        high = value.astype(BF16).astype(F32)
        row_hot = hot(SPAN, place // SPAN)
        lane_hot = hot(WIDE, lane_target(place)).astype(F32).astype(BF16)
        left = jnp.where(row_hot, high, 0.0).astype(BF16)
        right = jnp.where(row_hot, value - high, 0.0).astype(BF16)
        total = total + (dot_t(left, lane_hot) + dot_t(right, lane_hot))
    return total


def decode_kernel(groups, order, lists, out):
    low = order[0]
    for index in range(groups):
        lanes = slice(index * WIDE, (index + 1) * WIDE)
        out[:, lanes] = decode_group(index, low, lists, lists.shape[0])


def decode_last_kernel(groups, order, lists, held, out, squares):
    low = order[0]
    squared = jnp.zeros((8, WIDE), F32)
    for index in range(groups):
        lanes = slice(index * WIDE, (index + 1) * WIDE)
        total = held[:, lanes] + decode_group(index, low, lists, lists.shape[0])
        out[:, lanes] = total
        squared = squared + jnp.sum((total * total).reshape(8, 8, WIDE), axis=0)
    squares[...] = squared[:, :128] + squared[:, 128:]


def update_kernel(total, rows, high, low, out):
    for index in range(total.shape[1] // WIDE):
        lanes = slice(index * WIDE, (index + 1) * WIDE)
        out[:, lanes] = along_rows(rows[...], along_lanes(total[:, lanes], high[...], low[...]))


def apply_kernel(entries, weights, update, squares, out):
    scale = lax.rsqrt(jnp.sum(squares[...]) / entries + 1.0)
    out[...] = weights[...] - update[...] * scale


def call(kernel, shapes, flops, *args, smem=()):
    specs = [
        pl.BlockSpec(memory_space=pltpu.SMEM if at in smem else pltpu.VMEM)
        for at in range(len(args))
    ]
    out_specs = jax.tree.map(lambda _: pl.BlockSpec(memory_space=pltpu.VMEM), shapes)
    return pl.pallas_call(
        kernel,
        out_shape=shapes,
        in_specs=specs,
        out_specs=out_specs,
        cost_estimate=pl.CostEstimate(flops=flops, bytes_accessed=4 * SPAN * 3584, transcendentals=0),
        compiler_params=pltpu.CompilerParams(vmem_limit_bytes=24 * 1024 * 1024),
    )(*args)


def local(replicas, parts, gradient, momentum, weights, positions):
    table = dct_table()
    forward = row_operand(table), *lane_operand(table.T)
    inverse = row_operand(table.T), *lane_operand(table)
    forward = [jnp.asarray(part) for part in forward]
    inverse = [jnp.asarray(part) for part in inverse]
    height, width = weights.shape
    groups = width // WIDE
    place = positions.reshape(groups, 128)
    field = jax.ShapeDtypeStruct((height, width), F32)
    message, coefs = call(
        pick_kernel,
        (jax.ShapeDtypeStruct((1, 32, 128), F32), field),
        1 << 30,
        gradient,
        momentum,
        place,
        *forward,
    )
    new_momentum = call(
        momentum_kernel,
        jax.ShapeDtypeStruct(momentum.shape, F32),
        1 << 31,
        gradient,
        momentum,
        place,
        coefs,
        *inverse,
    )
    held = message
    bit = 1
    while 2 * bit < replicas:
        other = lax.ppermute(held, "dp", [(at, at ^ bit) for at in range(replicas)])
        held = jnp.concatenate([held, other], axis=0)
        bit *= 2
    order = (lax.axis_index("dp") % bit).reshape(1)
    other = lax.ppermute(held, "dp", [(at, at ^ bit) for at in range(replicas)])
    own_total = call(
        functools.partial(decode_kernel, groups), field, 1 << 30, order, held, smem=(0,)
    )
    total, squares = call(
        functools.partial(decode_last_kernel, groups),
        (field, jax.ShapeDtypeStruct((8, 128), F32)),
        1 << 30,
        order,
        other,
        own_total,
        smem=(0,),
    )
    update = call(update_kernel, field, 1 << 31, total, *inverse)
    step = 1
    while step < parts:
        squares = squares + lax.ppermute(squares, "mp", [(at, at ^ step) for at in range(parts)])
        step *= 2
    new_weights = call(
        functools.partial(apply_kernel, float(height * width * parts)),
        field,
        1 << 20,
        weights,
        update,
        squares,
    )
    return new_momentum, new_weights


def solution(mesh):
    placed = (P("dp", None, "mp"), P("dp", None, "mp"), P(None, "mp"), P("dp", None, "mp", None))
    return jax.shard_map(
        functools.partial(local, mesh.shape["dp"], mesh.shape["mp"]),
        mesh=mesh,
        in_specs=placed,
        out_specs=(P("dp", None, "mp"), P(None, "mp")),
        check_vma=False,
    )
```

```python
import functools

import jax
import jax.numpy as jnp
import numpy as np
from jax import lax
from jax.experimental import pallas as pl
from jax.experimental.pallas import tpu as pltpu
from jax.sharding import PartitionSpec as P

SPAN = 64
QUAD = 4
WIDE = SPAN * QUAD
F32 = jnp.float32
BF16 = jnp.bfloat16
VMEM_LIMIT = 24 * 1024 * 1024


def dct_table():
    column = np.arange(SPAN, dtype=np.float64)
    factor = np.where(column == 0, np.sqrt(1.0 / SPAN), np.sqrt(2.0 / SPAN))
    angle = np.pi * (2.0 * column[None, :] + 1.0) * column[:, None] / (2.0 * SPAN)
    return (factor[:, None] * np.cos(angle)).astype(np.float32)


def halves(table):
    high = table.astype(BF16)
    return high, (table - high.astype(np.float32)).astype(BF16)


def operands(table):
    high, low = halves(table)
    rows = np.concatenate([high, high, low, np.zeros_like(low)], axis=1)
    blocks = halves(np.kron(np.eye(QUAD, dtype=np.float32), table.T))
    return np.concatenate([rows, *blocks], axis=0)


def split(value):
    high = value.astype(BF16)
    return high, (value - high.astype(F32)).astype(BF16)


def dot(left, right):
    return lax.dot_general(left, right, (((1,), (0,)), ((), ())), preferred_element_type=F32)


def dot_t(left, right):
    return lax.dot_general(left, right, (((1,), (1,)), ((), ())), preferred_element_type=F32)


def row_table(tables):
    return tables[:SPAN, : 3 * SPAN]


def along_lanes(high, low, tables):
    high_table = tables[SPAN : SPAN + WIDE, :]
    low_table = tables[SPAN + WIDE :, :]
    return dot(high, high_table) + dot(low, high_table) + dot(high, low_table)


def put_rows(stack, lanes, value):
    high, low = split(value)
    stack[:SPAN, lanes] = high
    stack[SPAN : 2 * SPAN, lanes] = low
    stack[2 * SPAN :, lanes] = high


def lane_target(place):
    quarter = lax.broadcasted_iota(jnp.int32, place.shape, 1) // (128 // QUAD)
    return quarter * SPAN + place % SPAN


def counter(size):
    return lax.broadcasted_iota(jnp.int32, (size, 128), 0).astype(F32).astype(BF16).reshape(size // 16, 16, 128)


def same(count, wanted):
    row = jnp.broadcast_to(wanted, (16, wanted.shape[1])).astype(BF16)
    return count == row[None]


def ones_at(count, wanted):
    mask = same(count, wanted)
    return jnp.where(mask, jnp.ones((), BF16), jnp.zeros((), BF16)).reshape(-1, 128)


def value_at(count, wanted, value):
    row = jnp.broadcast_to(value, (16, 128)).astype(BF16)
    mask = same(count, wanted)
    return jnp.where(mask, jnp.broadcast_to(row[None], count.shape), jnp.zeros((), BF16)).reshape(-1, 128)


def pick_kernel(chunks, grad, mom, place, table, message, coefs, summed, g_buf, m_buf, p_buf, t_buf, turned, stack, high, low, lane_hot, sems):
    width = summed.shape[1]
    groups = width // WIDE
    step = width // chunks

    copies = [
        pltpu.make_async_copy(place, p_buf, sems.at[2 * chunks]),
        pltpu.make_async_copy(table, t_buf, sems.at[2 * chunks + 1]),
    ]
    for at in range(chunks):
        lanes = pl.ds(at * step, step)
        copies.append(pltpu.make_async_copy(grad.at[0, :, lanes], g_buf.at[:, lanes], sems.at[2 * at]))
        copies.append(pltpu.make_async_copy(mom.at[0, :, lanes], m_buf.at[:, lanes], sems.at[2 * at + 1]))
    for copy in copies:
        copy.start()
    copies[0].wait()
    turned[...] = jnp.transpose(p_buf[...])
    places = jnp.concatenate([turned[pl.ds(at, groups, stride=QUAD), :] for at in range(QUAD)], axis=1)
    message[...] = jnp.zeros_like(message)
    message[0, 16 : 16 + groups, :] = places.astype(F32)
    row_of = (places // SPAN).astype(F32)
    lane_of = lane_target(places).astype(F32)
    wide = counter(WIDE)
    for index in range(groups):
        lane_hot[index] = ones_at(wide, lane_of[index : index + 1])
    for at in range(chunks):
        lanes = slice(at * step, (at + 1) * step)
        copies[2 + 2 * at].wait()
        copies[3 + 2 * at].wait()
        total = 0.9 * m_buf[:, lanes] + g_buf[:, lanes].astype(F32)
        summed[:, lanes] = total
        put_rows(stack, lanes, total)
    copies[1].wait()
    along = dot(row_table(t_buf), stack[...])
    for index in range(groups):
        rows = slice(index * SPAN, (index + 1) * SPAN)
        high[rows, :], low[rows, :] = split(along[:, index * WIDE : (index + 1) * WIDE])
    coefs[...] = along_lanes(high[...], low[...], t_buf)
    grid = lax.broadcasted_iota(jnp.int32, (SPAN, 128), 0).astype(F32)
    for index in range(groups):
        coef_high, coef_low = split(coefs[index * SPAN : (index + 1) * SPAN, :])
        columns = dot(jnp.concatenate([coef_high, coef_low], axis=0), lane_hot[index])
        columns = columns[:SPAN] + columns[SPAN:]
        chosen = jnp.where(grid == row_of[index : index + 1], columns, 0.0)
        message[0, index : index + 1, :] = jnp.sum(chosen, axis=0, keepdims=True)


def inverse(high, low, tables, stack, groups):
    across = along_lanes(high[...], low[...], tables)
    for index in range(groups):
        lanes = slice(index * WIDE, (index + 1) * WIDE)
        put_rows(stack, lanes, across[index * SPAN : (index + 1) * SPAN, :])
    return dot(row_table(tables), stack[...])


def momentum_kernel(summed, message, coefs, tables, out, high, low, stack):
    groups = summed.shape[1] // WIDE
    places = message[0, 16 : 16 + groups, :].astype(jnp.int32)
    row_of = (places // SPAN).astype(F32)
    lane_of = lane_target(places).astype(F32)
    narrow, wide = counter(SPAN), counter(WIDE)
    for index in range(groups):
        rows = slice(index * SPAN, (index + 1) * SPAN)
        row_hot = ones_at(narrow, row_of[index : index + 1])
        lane_hot = ones_at(wide, lane_of[index : index + 1])
        own = coefs[rows, :] * dot_t(row_hot, lane_hot)
        high[rows, :], low[rows, :] = split(own)
    out[0] = summed[...] - inverse(high, low, tables, stack, groups)


def prepare(order, lists, groups, value_of, row_of, lane_of):
    for step in range(lists.shape[0]):
        which = step ^ order
        value_of[step] = lists[which, :groups, :]
        places = lists[which, 16 : 16 + groups, :].astype(jnp.int32)
        row_of[step] = (places // SPAN).astype(F32)
        lane_of[step] = lane_target(places).astype(F32)


def decode_group(index, narrow, wide, value_of, row_of, lane_of):
    left, right = [], []
    for step in range(value_of.shape[0]):
        value = value_of[step, index : index + 1, :]
        wanted = row_of[step, index : index + 1, :]
        high = value.astype(BF16).astype(F32)
        left.append(
            jnp.concatenate([value_at(narrow, wanted, high), value_at(narrow, wanted, value - high)], axis=0)
        )
        right.append(ones_at(wide, lane_of[step, index : index + 1, :]))
    total = dot_t(jnp.concatenate(left, axis=1), jnp.concatenate(right, axis=1))
    return total[:SPAN] + total[SPAN:]


def decode_kernel(groups, order, lists, out, value_of, row_of, lane_of):
    prepare(order[0], lists, groups, value_of, row_of, lane_of)
    narrow, wide = counter(SPAN), counter(WIDE)
    for index in range(groups):
        out[index * SPAN : (index + 1) * SPAN, :] = decode_group(index, narrow, wide, value_of, row_of, lane_of)


def decode_last_kernel(groups, order, lists, held, out, squares, value_of, row_of, lane_of):
    prepare(order[0], lists, groups, value_of, row_of, lane_of)
    narrow, wide = counter(SPAN), counter(WIDE)
    squared = jnp.zeros((8, WIDE), F32)
    for index in range(groups):
        rows = slice(index * SPAN, (index + 1) * SPAN)
        total = held[rows, :] + decode_group(index, narrow, wide, value_of, row_of, lane_of)
        out[rows, :] = total
        squared = squared + jnp.sum((total * total).reshape(8, 8, WIDE), axis=0)
    squares[...] = squared[:, :128] + squared[:, 128:]


def update_kernel(total, tables, out, high, low, stack):
    groups = total.shape[0] // SPAN
    for index in range(groups):
        rows = slice(index * SPAN, (index + 1) * SPAN)
        high[rows, :], low[rows, :] = split(total[rows, :])
    out[...] = inverse(high, low, tables, stack, groups)


def apply_kernel(entries, weights, update, squares, out):
    scale = lax.rsqrt(jnp.sum(squares[...]) / entries + 1.0)
    out[...] = weights[...] - update[...] * scale


def call(kernel, shapes, flops, *args, spaces=None, scratch=()):
    spaces = spaces or {}
    specs = [pl.BlockSpec(memory_space=spaces.get(at, pltpu.VMEM)) for at in range(len(args))]
    out_specs = jax.tree.map(lambda _: pl.BlockSpec(memory_space=pltpu.VMEM), shapes)
    return pl.pallas_call(
        kernel,
        out_shape=shapes,
        in_specs=specs,
        out_specs=out_specs,
        scratch_shapes=list(scratch),
        cost_estimate=pl.CostEstimate(flops=flops, bytes_accessed=1 << 20, transcendentals=0),
        compiler_params=pltpu.CompilerParams(vmem_limit_bytes=VMEM_LIMIT),
    )(*args)


def local(replicas, parts, gradient, momentum, weights, positions):
    table = dct_table()
    forward = jnp.asarray(operands(table))
    backward = jnp.asarray(operands(table.T))
    height, width = weights.shape
    groups = width // WIDE
    spans, kept = positions.shape[2:]
    chunks = 7
    field = jax.ShapeDtypeStruct((height, width), F32)
    tall = jax.ShapeDtypeStruct((groups * SPAN, WIDE), F32)
    half = pltpu.VMEM((groups * SPAN, WIDE), BF16)
    stack = pltpu.VMEM((3 * SPAN, width), BF16)
    message, coefs, summed = call(
        functools.partial(pick_kernel, chunks),
        (jax.ShapeDtypeStruct((1, 32, 128), F32), tall, field),
        1 << 30,
        pltpu.with_memory_space_constraint(gradient, pltpu.HBM),
        pltpu.with_memory_space_constraint(momentum, pltpu.HBM),
        pltpu.with_memory_space_constraint(jnp.swapaxes(positions[0, 0], 0, 1), pltpu.HBM),
        pltpu.with_memory_space_constraint(forward, pltpu.HBM),
        spaces={0: pltpu.HBM, 1: pltpu.HBM, 2: pltpu.HBM, 3: pltpu.HBM},
        scratch=(
            pltpu.VMEM((height, width), BF16),
            pltpu.VMEM((height, width), F32),
            pltpu.VMEM((kept, spans), jnp.int32),
            pltpu.VMEM(forward.shape, BF16),
            pltpu.VMEM((spans, kept), jnp.int32),
            stack,
            half,
            half,
            pltpu.VMEM((groups, WIDE, 128), BF16),
            pltpu.SemaphoreType.DMA((2 * chunks + 2,)),
        ),
    )
    new_momentum = call(
        momentum_kernel,
        jax.ShapeDtypeStruct(momentum.shape, F32),
        1 << 31,
        summed,
        message,
        coefs,
        backward,
        scratch=(half, half, stack),
    )
    held = message
    bit = 1
    while 2 * bit < replicas:
        other = lax.ppermute(held, "dp", [(at, at ^ bit) for at in range(replicas)])
        held = jnp.concatenate([held, other], axis=0)
        bit *= 2
    order = (lax.axis_index("dp") % bit).reshape(1)
    other = lax.ppermute(held, "dp", [(at, at ^ bit) for at in range(replicas)])
    tables = tuple(pltpu.VMEM((bit, groups, 128), F32) for _ in range(3))
    own_total = call(
        functools.partial(decode_kernel, groups),
        tall,
        1 << 30,
        order,
        held,
        spaces={0: pltpu.SMEM},
        scratch=tables,
    )
    total, squares = call(
        functools.partial(decode_last_kernel, groups),
        (tall, jax.ShapeDtypeStruct((8, 128), F32)),
        1 << 30,
        order,
        other,
        own_total,
        spaces={0: pltpu.SMEM},
        scratch=tables,
    )
    update = call(update_kernel, field, 1 << 31, total, backward, scratch=(half, half, stack))
    step = 1
    while step < parts:
        squares = squares + lax.ppermute(squares, "mp", [(at, at ^ step) for at in range(parts)])
        step *= 2
    new_weights = call(
        functools.partial(apply_kernel, float(height * width * parts)),
        field,
        1 << 20,
        weights,
        update,
        squares,
    )
    return new_momentum, new_weights


def solution(mesh):
    placed = (P("dp", None, "mp"), P("dp", None, "mp"), P(None, "mp"), P("dp", None, "mp", None))
    return jax.shard_map(
        functools.partial(local, mesh.shape["dp"], mesh.shape["mp"]),
        mesh=mesh,
        in_specs=placed,
        out_specs=(P("dp", None, "mp"), P(None, "mp")),
        check_vma=False,
    )
```

```python
import functools

import jax
import jax.numpy as jnp
import numpy as np
from jax import lax
from jax.experimental import pallas as pl
from jax.experimental.pallas import tpu as pltpu
from jax.sharding import PartitionSpec as P

SPAN = 64
QUAD = 4
WIDE = SPAN * QUAD
F32 = jnp.float32
BF16 = jnp.bfloat16
VMEM_LIMIT = 24 * 1024 * 1024


def dct_table():
    column = np.arange(SPAN, dtype=np.float64)
    factor = np.where(column == 0, np.sqrt(1.0 / SPAN), np.sqrt(2.0 / SPAN))
    angle = np.pi * (2.0 * column[None, :] + 1.0) * column[:, None] / (2.0 * SPAN)
    return (factor[:, None] * np.cos(angle)).astype(np.float32)


def halves(table):
    high = table.astype(BF16)
    return high, (table - high.astype(np.float32)).astype(BF16)


def operands(table):
    high, low = halves(table)
    rows = np.concatenate([high, high, low, np.zeros_like(low)], axis=1)
    blocks = halves(np.kron(np.eye(QUAD, dtype=np.float32), table.T))
    return np.concatenate([rows, *blocks], axis=0)


def split(value):
    high = value.astype(BF16)
    return high, (value - high.astype(F32)).astype(BF16)


def dot(left, right):
    return lax.dot_general(left, right, (((1,), (0,)), ((), ())), preferred_element_type=F32)


def dot_t(left, right):
    return lax.dot_general(left, right, (((1,), (1,)), ((), ())), preferred_element_type=F32)


def row_table(tables):
    return tables[:SPAN, : 3 * SPAN]


def along_lanes(high, low, tables):
    high_table = tables[SPAN : SPAN + WIDE, :]
    low_table = tables[SPAN + WIDE :, :]
    return dot(high, high_table) + dot(low, high_table) + dot(high, low_table)


def put_rows(stack, lanes, value):
    high, low = split(value)
    stack[:SPAN, lanes] = high
    stack[SPAN : 2 * SPAN, lanes] = low
    stack[2 * SPAN :, lanes] = high


def lane_target(place):
    quarter = lax.broadcasted_iota(jnp.int32, place.shape, 1) // (128 // QUAD)
    return quarter * SPAN + place % SPAN


def counter(size):
    return lax.broadcasted_iota(jnp.int32, (size, 128), 0).astype(F32).astype(BF16).reshape(size // 16, 16, 128)


def same(count, wanted):
    row = jnp.broadcast_to(wanted, (16, wanted.shape[1])).astype(BF16)
    return count == row[None]


def ones_at(count, wanted):
    mask = same(count, wanted)
    return jnp.where(mask, jnp.ones((), BF16), jnp.zeros((), BF16)).reshape(-1, 128)


def value_at(count, wanted, value):
    row = jnp.broadcast_to(value, (16, 128)).astype(BF16)
    mask = same(count, wanted)
    return jnp.where(mask, jnp.broadcast_to(row[None], count.shape), jnp.zeros((), BF16)).reshape(-1, 128)


def pick_kernel(chunks, grad, mom, place, table, message, summed, sides, column, g_buf, m_buf, p_buf, t_buf, turned, hots, sems):
    width = summed.shape[1]
    groups = width // WIDE
    step = width // chunks
    copies = [
        pltpu.make_async_copy(place, p_buf, sems.at[2 * chunks]),
        pltpu.make_async_copy(table, t_buf, sems.at[2 * chunks + 1]),
    ]
    for at in range(chunks):
        lanes = pl.ds(at * step, step)
        copies.append(pltpu.make_async_copy(grad.at[0, :, lanes], g_buf.at[:, lanes], sems.at[2 * at]))
        copies.append(pltpu.make_async_copy(mom.at[0, :, lanes], m_buf.at[:, lanes], sems.at[2 * at + 1]))
    for copy in copies:
        copy.start()
    narrow = counter(SPAN)
    lane = lax.broadcasted_iota(jnp.int32, (16, 128), 1) // (128 // QUAD)
    masks = [jnp.where(lane == at, 1.0, 0.0).astype(BF16) == jnp.ones((), BF16) for at in range(QUAD)]
    message[...] = jnp.zeros_like(message)
    copies[0].wait()
    turned[...] = jnp.transpose(p_buf[...])
    places = jnp.concatenate([turned[pl.ds(at, groups, stride=QUAD), :] for at in range(QUAD)], axis=1)
    message[0, 16 : 16 + groups, :] = places.astype(F32)
    row_of = (places // SPAN).astype(F32)
    column_of = (places % SPAN).astype(F32)
    for index in range(groups):
        hots[:, index * WIDE : index * WIDE + 128] = ones_at(narrow, column_of[index : index + 1])
        hots[:, index * WIDE + 128 : (index + 1) * WIDE] = ones_at(narrow, row_of[index : index + 1])
    copies[1].wait()
    chosen = dot(t_buf[...], hots[...])
    for index in range(groups):
        at = index * WIDE
        for half in range(2):
            tall = slice(half * SPAN, (half + 1) * SPAN)
            piece = chosen[tall, at : at + 128].astype(BF16).reshape(SPAN // 16, 16, 128)
            for quarter in range(QUAD):
                kept = jnp.where(masks[quarter][None], piece, jnp.zeros((), BF16)).reshape(SPAN, 128)
                sides[index, half, quarter * SPAN : (quarter + 1) * SPAN, :] = kept
        column[index] = chosen[:SPAN, at + 128 : at + WIDE] + chosen[SPAN:, at + 128 : at + WIDE]
    for at in range(chunks):
        lanes = slice(at * step, (at + 1) * step)
        copies[2 + 2 * at].wait()
        copies[3 + 2 * at].wait()
        total = 0.9 * m_buf[:, lanes] + g_buf[:, lanes].astype(F32)
        summed[:, lanes] = total
        for index in range(at * step // WIDE, (at + 1) * step // WIDE):
            inner = index * WIDE - at * step
            high, low = split(total[:, inner : inner + WIDE])
            both = dot(jnp.concatenate([high, low], axis=0), sides[index, 0])
            values = both[:SPAN] + both[SPAN:] + dot(high, sides[index, 1])
            message[0, index : index + 1, :] = jnp.sum(values * column[index], axis=0, keepdims=True)


def inverse(high, low, tables, stack, groups):
    across = along_lanes(high[...], low[...], tables)
    for index in range(groups):
        lanes = slice(index * WIDE, (index + 1) * WIDE)
        put_rows(stack, lanes, across[index * SPAN : (index + 1) * SPAN, :])
    return dot(row_table(tables), stack[...])


def momentum_kernel(message, summed, sides, column, out, buf, sems):
    groups = column.shape[0]
    copies = []
    for index in range(groups):
        lanes = pl.ds(index * WIDE, WIDE)
        high, low = split(column[index] * message[0, index : index + 1, :])
        both = dot_t(jnp.concatenate([high, low], axis=0), sides[index, 0])
        buf[:, lanes] = summed[:, lanes] - (both[:SPAN] + both[SPAN:] + dot_t(high, sides[index, 1]))
        copies.append(pltpu.make_async_copy(buf.at[:, lanes], out.at[0, :, lanes], sems.at[index]))
        copies[-1].start()
    for copy in copies:
        copy.wait()


def prepare(order, lists, groups, value_of, row_of, lane_of):
    shape = (groups, 128)
    lane = lax.broadcasted_iota(jnp.int32, shape, 1)
    lower = lane < SPAN
    for step in range(0, lists.shape[0], 2):
        parts = []
        for which in (step ^ order, (step + 1) ^ order):
            places = lists[which, 16 : 16 + groups, :].astype(jnp.int32)
            target = (lane // (128 // QUAD)) % 2 * SPAN + places % SPAN
            parts.append((lists[which, :groups, :], (places // SPAN).astype(F32), target.astype(F32)))
        for out, first, second in zip((value_of, row_of, lane_of), *parts):
            out[step] = jnp.where(lower, first, pltpu.roll(second, SPAN, 1))
            out[step + 1] = jnp.where(lower, pltpu.roll(first, SPAN, 1), second)


def decode_group(index, narrow, wide, value_of, row_of, lane_of):
    pairs = []
    for pair in range(2):
        left, right = [], []
        for step in range(pair, value_of.shape[0], 2):
            value = value_of[step, index : index + 1, :]
            wanted = row_of[step, index : index + 1, :]
            high = value.astype(BF16).astype(F32)
            left.append(
                jnp.concatenate([value_at(narrow, wanted, high), value_at(narrow, wanted, value - high)], axis=0)
            )
            right.append(ones_at(wide, lane_of[step, index : index + 1, :]))
        total = dot_t(jnp.concatenate(left, axis=1), jnp.concatenate(right, axis=1))
        pairs.append(total[:SPAN] + total[SPAN:])
    return jnp.concatenate(pairs, axis=1)


def decode_kernel(groups, order, lists, out, value_of, row_of, lane_of):
    prepare(order[0], lists, groups, value_of, row_of, lane_of)
    narrow, wide = counter(SPAN), counter(2 * SPAN)
    for index in range(groups):
        out[index * SPAN : (index + 1) * SPAN, :] = decode_group(index, narrow, wide, value_of, row_of, lane_of)


def decode_last_kernel(groups, order, lists, held, out, squares, value_of, row_of, lane_of):
    prepare(order[0], lists, groups, value_of, row_of, lane_of)
    narrow, wide = counter(SPAN), counter(2 * SPAN)
    squared = jnp.zeros((8, WIDE), F32)
    for index in range(groups):
        rows = slice(index * SPAN, (index + 1) * SPAN)
        total = held[rows, :] + decode_group(index, narrow, wide, value_of, row_of, lane_of)
        out[rows, :] = total
        squared = squared + jnp.sum((total * total).reshape(8, 8, WIDE), axis=0)
    squares[...] = squared[:, :128] + squared[:, 128:]


def update_kernel(total, tables, out, high, low, stack):
    groups = total.shape[0] // SPAN
    for index in range(groups):
        rows = slice(index * SPAN, (index + 1) * SPAN)
        high[rows, :], low[rows, :] = split(total[rows, :])
    out[...] = inverse(high, low, tables, stack, groups)


def apply_kernel(entries, chunks, weights, update, squares, out, buf, sems):
    total = jnp.sum(jnp.sum(squares[...], axis=0, keepdims=True), axis=1, keepdims=True)
    scale = lax.rsqrt(total / entries + 1.0)
    step = update.shape[0] // chunks
    copies = []
    for at in range(chunks):
        rows = pl.ds(at * step, step)
        buf[rows, :] = weights[rows, :] - update[rows, :] * scale
        copies.append(pltpu.make_async_copy(buf.at[rows, :], out.at[rows, :], sems.at[at]))
        copies[-1].start()
    for copy in copies:
        copy.wait()


def call(kernel, shapes, flops, *args, spaces=None, scratch=(), space=pltpu.VMEM):
    spaces = spaces or {}
    specs = [pl.BlockSpec(memory_space=spaces.get(at, pltpu.VMEM)) for at in range(len(args))]
    out_specs = jax.tree.map(lambda _: pl.BlockSpec(memory_space=space), shapes)
    return pl.pallas_call(
        kernel,
        out_shape=shapes,
        in_specs=specs,
        out_specs=out_specs,
        scratch_shapes=list(scratch),
        cost_estimate=pl.CostEstimate(flops=flops, bytes_accessed=1 << 20, transcendentals=0),
        compiler_params=pltpu.CompilerParams(vmem_limit_bytes=VMEM_LIMIT),
    )(*args)


def local(replicas, parts, gradient, momentum, weights, positions):
    table = dct_table()
    columns = jnp.asarray(np.concatenate(halves(table.T), axis=0))
    backward = jnp.asarray(operands(table.T))
    height, width = weights.shape
    groups = width // WIDE
    spans, kept = positions.shape[2:]
    chunks = 1
    field = jax.ShapeDtypeStruct((height, width), F32)
    tall = jax.ShapeDtypeStruct((groups * SPAN, WIDE), F32)
    half = pltpu.VMEM((groups * SPAN, WIDE), BF16)
    stack = pltpu.VMEM((3 * SPAN, width), BF16)
    message, summed, sides, column = call(
        functools.partial(pick_kernel, chunks),
        (
            jax.ShapeDtypeStruct((1, 32, 128), F32),
            field,
            jax.ShapeDtypeStruct((groups, 2, WIDE, 128), BF16),
            jax.ShapeDtypeStruct((groups, SPAN, 128), F32),
        ),
        1 << 30,
        pltpu.with_memory_space_constraint(gradient, pltpu.HBM),
        pltpu.with_memory_space_constraint(momentum, pltpu.HBM),
        pltpu.with_memory_space_constraint(jnp.swapaxes(positions[0, 0], 0, 1), pltpu.HBM),
        pltpu.with_memory_space_constraint(columns, pltpu.HBM),
        spaces={0: pltpu.HBM, 1: pltpu.HBM, 2: pltpu.HBM, 3: pltpu.HBM},
        scratch=(
            pltpu.VMEM((height, width), BF16),
            pltpu.VMEM((height, width), F32),
            pltpu.VMEM((kept, spans), jnp.int32),
            pltpu.VMEM(columns.shape, BF16),
            pltpu.VMEM((spans, kept), jnp.int32),
            pltpu.VMEM((SPAN, width), BF16),
            pltpu.SemaphoreType.DMA((2 * chunks + 2,)),
        ),
    )
    new_momentum = call(
        momentum_kernel,
        jax.ShapeDtypeStruct(momentum.shape, F32),
        1 << 31,
        message,
        summed,
        sides,
        column,
        space=pltpu.HBM,
        scratch=(pltpu.VMEM((height, width), F32), pltpu.SemaphoreType.DMA((groups,))),
    )
    held = message
    bit = 1
    fillers = [new_momentum]
    while 2 * bit < replicas:
        other = lax.ppermute(held, "dp", [(at, at ^ bit) for at in range(replicas)])
        held = jnp.concatenate([held, other], axis=0)
        if fillers:
            held, _ = lax.optimization_barrier((held, fillers.pop(0)))
        bit *= 2
    order = (lax.axis_index("dp") % bit).reshape(1)
    other = lax.ppermute(held, "dp", [(at, at ^ bit) for at in range(replicas)])
    tables = tuple(pltpu.VMEM((bit, groups, 128), F32) for _ in range(3))
    own_total = call(
        functools.partial(decode_kernel, groups),
        tall,
        1 << 30,
        order,
        held,
        spaces={0: pltpu.SMEM},
        scratch=tables,
    )
    total, squares = call(
        functools.partial(decode_last_kernel, groups),
        (tall, jax.ShapeDtypeStruct((8, 128), F32)),
        1 << 30,
        order,
        other,
        own_total,
        spaces={0: pltpu.SMEM},
        scratch=tables,
    )
    update = call(update_kernel, field, 1 << 31, total, backward, scratch=(half, half, stack))
    step = 1
    while step < parts:
        squares = squares + lax.ppermute(squares, "mp", [(at, at ^ step) for at in range(parts)])
        step *= 2
    new_weights = call(
        functools.partial(apply_kernel, float(height * width * parts), 4),
        field,
        1 << 20,
        weights,
        update,
        squares,
        space=pltpu.HBM,
        scratch=(pltpu.VMEM((height, width), F32), pltpu.SemaphoreType.DMA((4,))),
    )
    return new_momentum, new_weights


def solution(mesh):
    placed = (P("dp", None, "mp"), P("dp", None, "mp"), P(None, "mp"), P("dp", None, "mp", None))
    return jax.shard_map(
        functools.partial(local, mesh.shape["dp"], mesh.shape["mp"]),
        mesh=mesh,
        in_specs=placed,
        out_specs=(P("dp", None, "mp"), P(None, "mp")),
        check_vma=False,
    )
```

```python
import functools

import jax
import jax.numpy as jnp
import numpy as np
from jax import lax
from jax.experimental import pallas as pl
from jax.experimental.pallas import tpu as pltpu
from jax.sharding import PartitionSpec as P

SPAN = 64
QUAD = 4
WIDE = SPAN * QUAD
F32 = jnp.float32
BF16 = jnp.bfloat16
VMEM_LIMIT = 24 * 1024 * 1024


def dct_table():
    column = np.arange(SPAN, dtype=np.float64)
    factor = np.where(column == 0, np.sqrt(1.0 / SPAN), np.sqrt(2.0 / SPAN))
    angle = np.pi * (2.0 * column[None, :] + 1.0) * column[:, None] / (2.0 * SPAN)
    return (factor[:, None] * np.cos(angle)).astype(np.float32)


def halves(table):
    high = table.astype(BF16)
    return high, (table - high.astype(np.float32)).astype(BF16)


def operands(table):
    high, low = halves(table)
    rows = np.concatenate([high, high, low, np.zeros_like(low)], axis=1)
    blocks = halves(np.kron(np.eye(QUAD, dtype=np.float32), table.T))
    return np.concatenate([rows, *blocks], axis=0)


def split(value):
    high = value.astype(BF16)
    return high, (value - high.astype(F32)).astype(BF16)


def dot(left, right):
    return lax.dot_general(left, right, (((1,), (0,)), ((), ())), preferred_element_type=F32)


def dot_t(left, right):
    return lax.dot_general(left, right, (((1,), (1,)), ((), ())), preferred_element_type=F32)


def row_table(tables):
    return tables[:SPAN, : 3 * SPAN]


def along_lanes(high, low, tables):
    high_table = tables[SPAN : SPAN + WIDE, :]
    low_table = tables[SPAN + WIDE :, :]
    return dot(high, high_table) + dot(low, high_table) + dot(high, low_table)


def put_rows(stack, lanes, value):
    high, low = split(value)
    stack[:SPAN, lanes] = high
    stack[SPAN : 2 * SPAN, lanes] = low
    stack[2 * SPAN :, lanes] = high


def lane_target(place):
    quarter = lax.broadcasted_iota(jnp.int32, place.shape, 1) // (128 // QUAD)
    return quarter * SPAN + place % SPAN


def counter(size):
    return lax.broadcasted_iota(jnp.int32, (size, 128), 0).astype(F32).astype(BF16).reshape(size // 16, 16, 128)


def same(count, wanted):
    row = jnp.broadcast_to(wanted, (16, wanted.shape[1])).astype(BF16)
    return count == row[None]


def ones_at(count, wanted):
    mask = same(count, wanted)
    return jnp.where(mask, jnp.ones((), BF16), jnp.zeros((), BF16)).reshape(-1, 128)


def value_at(count, wanted, value):
    row = jnp.broadcast_to(value, (16, 128)).astype(BF16)
    mask = same(count, wanted)
    return jnp.where(mask, jnp.broadcast_to(row[None], count.shape), jnp.zeros((), BF16)).reshape(-1, 128)


def pick_kernel(chunks, grad, mom, place, table, message, summed, sides, column, g_buf, m_buf, p_buf, t_buf, turned, hots, sems):
    width = summed.shape[1]
    groups = width // WIDE
    step = width // chunks
    copies = [
        pltpu.make_async_copy(place, p_buf, sems.at[2 * chunks]),
        pltpu.make_async_copy(table, t_buf, sems.at[2 * chunks + 1]),
    ]
    for at in range(chunks):
        lanes = pl.ds(at * step, step)
        copies.append(pltpu.make_async_copy(grad.at[0, :, lanes], g_buf.at[:, lanes], sems.at[2 * at]))
        copies.append(pltpu.make_async_copy(mom.at[0, :, lanes], m_buf.at[:, lanes], sems.at[2 * at + 1]))
    for copy in copies:
        copy.start()
    narrow = counter(SPAN)
    lane = lax.broadcasted_iota(jnp.int32, (16, 128), 1) // (128 // QUAD)
    masks = [jnp.where(lane == at, 1.0, 0.0).astype(BF16) == jnp.ones((), BF16) for at in range(QUAD)]
    message[...] = jnp.zeros_like(message)
    copies[0].wait()
    turned[...] = jnp.transpose(p_buf[...])
    places = jnp.concatenate([turned[pl.ds(at, groups, stride=QUAD), :] for at in range(QUAD)], axis=1)
    message[0, 16 : 16 + groups, :] = places.astype(F32)
    row_of = (places // SPAN).astype(F32)
    column_of = (places % SPAN).astype(F32)
    for index in range(groups):
        hots[:, index * WIDE : index * WIDE + 128] = ones_at(narrow, column_of[index : index + 1])
        hots[:, index * WIDE + 128 : (index + 1) * WIDE] = ones_at(narrow, row_of[index : index + 1])
    copies[1].wait()
    chosen = dot(t_buf[...], hots[...])
    for index in range(groups):
        at = index * WIDE
        for half in range(2):
            tall = slice(half * SPAN, (half + 1) * SPAN)
            piece = chosen[tall, at : at + 128].astype(BF16).reshape(SPAN // 16, 16, 128)
            for quarter in range(QUAD):
                kept = jnp.where(masks[quarter][None], piece, jnp.zeros((), BF16)).reshape(SPAN, 128)
                sides[index, quarter * SPAN : (quarter + 1) * SPAN, half * 128 : (half + 1) * 128] = kept
        column[index] = chosen[:SPAN, at + 128 : at + WIDE] + chosen[SPAN:, at + 128 : at + WIDE]
    for at in range(chunks):
        lanes = slice(at * step, (at + 1) * step)
        copies[2 + 2 * at].wait()
        copies[3 + 2 * at].wait()
        total = 0.9 * m_buf[:, lanes] + g_buf[:, lanes].astype(F32)
        summed[:, lanes] = total
        for index in range(at * step // WIDE, (at + 1) * step // WIDE):
            inner = index * WIDE - at * step
            high, low = split(total[:, inner : inner + WIDE])
            both = dot(jnp.concatenate([high, low], axis=0), sides[index])
            values = both[:SPAN, :128] + both[SPAN:, :128] + both[:SPAN, 128:]
            message[0, index : index + 1, :] = jnp.sum(values * column[index], axis=0, keepdims=True)


def inverse(high, low, tables, stack, groups):
    across = along_lanes(high[...], low[...], tables)
    for index in range(groups):
        lanes = slice(index * WIDE, (index + 1) * WIDE)
        put_rows(stack, lanes, across[index * SPAN : (index + 1) * SPAN, :])
    return dot(row_table(tables), stack[...])


def momentum_kernel(message, summed, sides, column, out, buf, sems):
    groups = column.shape[0]
    copies = []
    for index in range(groups):
        lanes = pl.ds(index * WIDE, WIDE)
        high, low = split(column[index] * message[0, index : index + 1, :])
        left = jnp.concatenate(
            [jnp.concatenate([high, high], axis=1), jnp.concatenate([low, jnp.zeros_like(low)], axis=1)], axis=0
        )
        both = dot_t(left, sides[index])
        buf[:, lanes] = summed[:, lanes] - (both[:SPAN] + both[SPAN:])
        copies.append(pltpu.make_async_copy(buf.at[:, lanes], out.at[0, :, lanes], sems.at[index]))
        copies[-1].start()
    for copy in copies:
        copy.wait()


def prepare(order, lists, groups, tables):
    shape = (groups, 128)
    lane = lax.broadcasted_iota(jnp.int32, shape, 1)
    lower = lane < SPAN
    for step in range(0, lists.shape[0], 2):
        parts = []
        for which in (step ^ order, (step + 1) ^ order):
            value = lists[which, :groups, :]
            high = value.astype(BF16).astype(F32)
            places = lists[which, 16 : 16 + groups, :].astype(jnp.int32)
            target = (lane // (128 // QUAD)) % 2 * SPAN + places % SPAN
            parts.append((high, value - high, (places // SPAN).astype(F32), target.astype(F32)))
        for out, first, second in zip(tables, *parts):
            out[step] = jnp.where(lower, first, pltpu.roll(second, SPAN, 1))
            out[step + 1] = jnp.where(lower, pltpu.roll(first, SPAN, 1), second)


def decode_group(index, narrow, wide, tables):
    pairs = []
    for pair in range(2):
        left, right = [], []
        for step in range(pair, tables[0].shape[0], 2):
            high, low, row, target = (table[step, index : index + 1, :] for table in tables)
            left.append(jnp.concatenate([value_at(narrow, row, high), value_at(narrow, row, low)], axis=0))
            right.append(ones_at(wide, target))
        total = dot_t(jnp.concatenate(left, axis=1), jnp.concatenate(right, axis=1))
        pairs.append(total[:SPAN] + total[SPAN:])
    return jnp.concatenate(pairs, axis=1)


def decode_kernel(groups, order, lists, out, *tables):
    prepare(order[0], lists, groups, tables)
    narrow, wide = counter(SPAN), counter(2 * SPAN)
    for index in range(groups):
        out[index * SPAN : (index + 1) * SPAN, :] = decode_group(index, narrow, wide, tables)


def decode_last_kernel(groups, order, lists, held, out, squares, *tables):
    prepare(order[0], lists, groups, tables)
    narrow, wide = counter(SPAN), counter(2 * SPAN)
    squared = jnp.zeros((8, WIDE), F32)
    for index in range(groups):
        rows = slice(index * SPAN, (index + 1) * SPAN)
        total = held[rows, :] + decode_group(index, narrow, wide, tables)
        out[rows, :] = total
        squared = squared + jnp.sum((total * total).reshape(8, 8, WIDE), axis=0)
    squares[...] = squared[:, :128] + squared[:, 128:]


def update_kernel(total, tables, out, high, low, stack):
    groups = total.shape[0] // SPAN
    for index in range(groups):
        rows = slice(index * SPAN, (index + 1) * SPAN)
        high[rows, :], low[rows, :] = split(total[rows, :])
    out[...] = inverse(high, low, tables, stack, groups)


def apply_kernel(entries, chunks, weights, update, squares, out, buf, sems):
    total = jnp.sum(jnp.sum(squares[...], axis=0, keepdims=True), axis=1, keepdims=True)
    scale = lax.rsqrt(total / entries + 1.0)
    step = update.shape[0] // chunks
    copies = []
    for at in range(chunks):
        rows = pl.ds(at * step, step)
        buf[rows, :] = weights[rows, :] - update[rows, :] * scale
        copies.append(pltpu.make_async_copy(buf.at[rows, :], out.at[rows, :], sems.at[at]))
        copies[-1].start()
    for copy in copies:
        copy.wait()


def call(kernel, shapes, flops, *args, spaces=None, scratch=(), space=pltpu.VMEM):
    spaces = spaces or {}
    specs = [pl.BlockSpec(memory_space=spaces.get(at, pltpu.VMEM)) for at in range(len(args))]
    out_specs = jax.tree.map(lambda _: pl.BlockSpec(memory_space=space), shapes)
    return pl.pallas_call(
        kernel,
        out_shape=shapes,
        in_specs=specs,
        out_specs=out_specs,
        scratch_shapes=list(scratch),
        cost_estimate=pl.CostEstimate(flops=flops, bytes_accessed=1 << 20, transcendentals=0),
        compiler_params=pltpu.CompilerParams(vmem_limit_bytes=VMEM_LIMIT),
    )(*args)


def local(replicas, parts, gradient, momentum, weights, positions):
    table = dct_table()
    columns = jnp.asarray(np.concatenate(halves(table.T), axis=0))
    backward = jnp.asarray(operands(table.T))
    height, width = weights.shape
    groups = width // WIDE
    spans, kept = positions.shape[2:]
    chunks = 1
    field = jax.ShapeDtypeStruct((height, width), F32)
    tall = jax.ShapeDtypeStruct((groups * SPAN, WIDE), F32)
    half = pltpu.VMEM((groups * SPAN, WIDE), BF16)
    stack = pltpu.VMEM((3 * SPAN, width), BF16)
    message, summed, sides, column = call(
        functools.partial(pick_kernel, chunks),
        (
            jax.ShapeDtypeStruct((1, 32, 128), F32),
            field,
            jax.ShapeDtypeStruct((groups, WIDE, 2 * 128), BF16),
            jax.ShapeDtypeStruct((groups, SPAN, 128), F32),
        ),
        1 << 30,
        pltpu.with_memory_space_constraint(gradient, pltpu.HBM),
        pltpu.with_memory_space_constraint(momentum, pltpu.HBM),
        pltpu.with_memory_space_constraint(jnp.swapaxes(positions[0, 0], 0, 1), pltpu.HBM),
        pltpu.with_memory_space_constraint(columns, pltpu.HBM),
        spaces={0: pltpu.HBM, 1: pltpu.HBM, 2: pltpu.HBM, 3: pltpu.HBM},
        scratch=(
            pltpu.VMEM((height, width), BF16),
            pltpu.VMEM((height, width), F32),
            pltpu.VMEM((kept, spans), jnp.int32),
            pltpu.VMEM(columns.shape, BF16),
            pltpu.VMEM((spans, kept), jnp.int32),
            pltpu.VMEM((SPAN, width), BF16),
            pltpu.SemaphoreType.DMA((2 * chunks + 2,)),
        ),
    )
    new_momentum = call(
        momentum_kernel,
        jax.ShapeDtypeStruct(momentum.shape, F32),
        1 << 31,
        message,
        summed,
        sides,
        column,
        space=pltpu.HBM,
        scratch=(pltpu.VMEM((height, width), F32), pltpu.SemaphoreType.DMA((groups,))),
    )
    held = message
    bit = 1
    fillers = [new_momentum]
    while 2 * bit < replicas:
        other = lax.ppermute(held, "dp", [(at, at ^ bit) for at in range(replicas)])
        held = jnp.concatenate([held, other], axis=0)
        if fillers:
            held, _ = lax.optimization_barrier((held, fillers.pop(0)))
        bit *= 2
    order = (lax.axis_index("dp") % bit).reshape(1)
    other = lax.ppermute(held, "dp", [(at, at ^ bit) for at in range(replicas)])
    tables = tuple(pltpu.VMEM((bit, groups, 128), F32) for _ in range(4))
    own_total = call(
        functools.partial(decode_kernel, groups),
        tall,
        1 << 30,
        order,
        held,
        spaces={0: pltpu.SMEM},
        scratch=tables,
    )
    total, squares = call(
        functools.partial(decode_last_kernel, groups),
        (tall, jax.ShapeDtypeStruct((8, 128), F32)),
        1 << 30,
        order,
        other,
        own_total,
        spaces={0: pltpu.SMEM},
        scratch=tables,
    )
    update = call(update_kernel, field, 1 << 31, total, backward, scratch=(half, half, stack))
    step = 1
    while step < parts:
        flip = 2 * step - 1
        squares = squares + lax.ppermute(squares, "mp", [(at, at ^ flip) for at in range(parts)])
        step *= 2
    new_weights = call(
        functools.partial(apply_kernel, float(height * width * parts), 4),
        field,
        1 << 20,
        weights,
        update,
        squares,
        space=pltpu.HBM,
        scratch=(pltpu.VMEM((height, width), F32), pltpu.SemaphoreType.DMA((4,))),
    )
    return new_momentum, new_weights


def solution(mesh):
    placed = (P("dp", None, "mp"), P("dp", None, "mp"), P(None, "mp"), P("dp", None, "mp", None))
    return jax.shard_map(
        functools.partial(local, mesh.shape["dp"], mesh.shape["mp"]),
        mesh=mesh,
        in_specs=placed,
        out_specs=(P("dp", None, "mp"), P(None, "mp")),
        check_vma=False,
    )
```

```python
import functools

import jax
import jax.numpy as jnp
import numpy as np
from jax import lax
from jax.experimental import pallas as pl
from jax.experimental.pallas import tpu as pltpu
from jax.sharding import PartitionSpec as P

SPAN = 64
QUAD = 4
WIDE = SPAN * QUAD
SHIFT = 6
F32 = jnp.float32
BF16 = jnp.bfloat16
VMEM_LIMIT = 24 * 1024 * 1024


def dct_table():
    column = np.arange(SPAN, dtype=np.float64)
    factor = np.where(column == 0, np.sqrt(1.0 / SPAN), np.sqrt(2.0 / SPAN))
    angle = np.pi * (2.0 * column[None, :] + 1.0) * column[:, None] / (2.0 * SPAN)
    return (factor[:, None] * np.cos(angle)).astype(np.float32)


def halves(table):
    high = table.astype(BF16)
    return high, (table - high.astype(np.float32)).astype(BF16)


def operands(table):
    high, low = halves(table)
    rows = np.concatenate([high, high, low, np.zeros_like(low)], axis=1)
    blocks = halves(np.kron(np.eye(QUAD, dtype=np.float32), table.T))
    return np.concatenate([rows, *blocks], axis=0)


def split(value):
    high = value.astype(BF16)
    return high, (value - high.astype(F32)).astype(BF16)


def dot(left, right):
    return lax.dot_general(left, right, (((1,), (0,)), ((), ())), preferred_element_type=F32)


def dot_t(left, right):
    return lax.dot_general(left, right, (((1,), (1,)), ((), ())), preferred_element_type=F32)


def row_table(tables):
    return tables[:SPAN, : 3 * SPAN]


def along_lanes(high, low, tables):
    high_table = tables[SPAN : SPAN + WIDE, :]
    low_table = tables[SPAN + WIDE :, :]
    return dot(high, high_table) + dot(low, high_table) + dot(high, low_table)


def put_rows(stack, lanes, value):
    high, low = split(value)
    stack[:SPAN, lanes] = high
    stack[SPAN : 2 * SPAN, lanes] = low
    stack[2 * SPAN :, lanes] = high


def lane_target(place):
    quarter = lax.broadcasted_iota(jnp.int32, place.shape, 1) // (128 // QUAD)
    return quarter * SPAN + (place & (SPAN - 1))


def counter(size):
    return lax.broadcasted_iota(jnp.int32, (size, 128), 0).astype(F32).astype(BF16).reshape(size // 16, 16, 128)


def same(count, wanted):
    row = jnp.broadcast_to(wanted, (16, wanted.shape[1])).astype(BF16)
    return count == row[None]


def ones_at(count, wanted):
    mask = same(count, wanted)
    return jnp.where(mask, jnp.ones((), BF16), jnp.zeros((), BF16)).reshape(-1, 128)


def value_at(count, wanted, value):
    row = jnp.broadcast_to(value, (16, 128)).astype(BF16)
    mask = same(count, wanted)
    return jnp.where(mask, jnp.broadcast_to(row[None], count.shape), jnp.zeros((), BF16)).reshape(-1, 128)


def pick_kernel(chunks, grad, mom, place, table, message, summed, sides, column, g_buf, m_buf, p_buf, t_buf, turned, hots, sems):
    width = summed.shape[1]
    groups = width // WIDE
    step = width // chunks
    copies = [
        pltpu.make_async_copy(place, p_buf, sems.at[2 * chunks]),
        pltpu.make_async_copy(table, t_buf, sems.at[2 * chunks + 1]),
    ]
    for at in range(chunks):
        lanes = pl.ds(at * step, step)
        copies.append(pltpu.make_async_copy(grad.at[0, :, lanes], g_buf.at[:, lanes], sems.at[2 * at]))
        copies.append(pltpu.make_async_copy(mom.at[0, :, lanes], m_buf.at[:, lanes], sems.at[2 * at + 1]))
    for copy in copies:
        copy.start()
    narrow = counter(SPAN)
    lane = lax.broadcasted_iota(jnp.int32, (16, 128), 1) // (128 // QUAD)
    masks = [jnp.where(lane == at, 1.0, 0.0).astype(BF16) == jnp.ones((), BF16) for at in range(QUAD)]
    message[...] = jnp.zeros_like(message)
    copies[0].wait()
    turned[...] = jnp.transpose(p_buf[...])
    places = jnp.concatenate([turned[pl.ds(at, groups, stride=QUAD), :] for at in range(QUAD)], axis=1)
    message[0, 16 : 16 + groups, :] = places.astype(F32)
    row_of = (places >> SHIFT).astype(F32)
    column_of = ((places & (SPAN - 1))).astype(F32)
    for index in range(groups):
        hots[:, index * WIDE : index * WIDE + 128] = ones_at(narrow, column_of[index : index + 1])
        hots[:, index * WIDE + 128 : (index + 1) * WIDE] = ones_at(narrow, row_of[index : index + 1])
    copies[1].wait()
    chosen = dot(t_buf[...], hots[...])
    for index in range(groups):
        at = index * WIDE
        for half in range(2):
            tall = slice(half * SPAN, (half + 1) * SPAN)
            piece = chosen[tall, at : at + 128].astype(BF16).reshape(SPAN // 16, 16, 128)
            for quarter in range(QUAD):
                kept = jnp.where(masks[quarter][None], piece, jnp.zeros((), BF16)).reshape(SPAN, 128)
                sides[index, quarter * SPAN : (quarter + 1) * SPAN, half * 128 : (half + 1) * 128] = kept
        column[index] = chosen[:SPAN, at + 128 : at + WIDE] + chosen[SPAN:, at + 128 : at + WIDE]
    for at in range(chunks):
        lanes = slice(at * step, (at + 1) * step)
        copies[2 + 2 * at].wait()
        copies[3 + 2 * at].wait()
        total = 0.9 * m_buf[:, lanes] + g_buf[:, lanes].astype(F32)
        summed[:, lanes] = total
        for index in range(at * step // WIDE, (at + 1) * step // WIDE):
            inner = index * WIDE - at * step
            high, low = split(total[:, inner : inner + WIDE])
            both = dot(jnp.concatenate([high, low], axis=0), sides[index])
            values = both[:SPAN, :128] + both[SPAN:, :128] + both[:SPAN, 128:]
            message[0, index : index + 1, :] = jnp.sum(values * column[index], axis=0, keepdims=True)


def inverse(high, low, tables, stack, groups):
    across = along_lanes(high[...], low[...], tables)
    for index in range(groups):
        lanes = slice(index * WIDE, (index + 1) * WIDE)
        put_rows(stack, lanes, across[index * SPAN : (index + 1) * SPAN, :])
    return dot(row_table(tables), stack[...])


def momentum_kernel(message, summed, sides, column, out, buf, sems):
    groups = column.shape[0]
    copies = []
    for index in range(groups):
        lanes = pl.ds(index * WIDE, WIDE)
        high, low = split(column[index] * message[0, index : index + 1, :])
        left = jnp.concatenate(
            [jnp.concatenate([high, high], axis=1), jnp.concatenate([low, jnp.zeros_like(low)], axis=1)], axis=0
        )
        both = dot_t(left, sides[index])
        buf[:, lanes] = summed[:, lanes] - (both[:SPAN] + both[SPAN:])
        copies.append(pltpu.make_async_copy(buf.at[:, lanes], out.at[0, :, lanes], sems.at[index]))
        copies[-1].start()
    for copy in copies:
        copy.wait()


def prepare(lists, groups, tables):
    order = lax.axis_index("dp") & (lists.shape[0] - 1)
    shape = (groups, 128)
    lane = lax.broadcasted_iota(jnp.int32, shape, 1)
    lower = lane < SPAN
    span = ((lane >> 5) & 1) * SPAN
    for step in range(0, lists.shape[0], 2):
        parts = []
        for which in (step ^ order, (step + 1) ^ order):
            value = lists[which, :groups, :]
            high = value.astype(BF16).astype(F32)
            places = lists[which, 16 : 16 + groups, :].astype(jnp.int32)
            target = span + (places & (SPAN - 1))
            parts.append((high, value - high, (places >> SHIFT).astype(F32), target.astype(F32)))
        for out, first, second in zip(tables, *parts):
            out[step] = jnp.where(lower, first, pltpu.roll(second, SPAN, 1))
            out[step + 1] = jnp.where(lower, pltpu.roll(first, SPAN, 1), second)


def decode_group(index, narrow, wide, tables):
    pairs = []
    for pair in range(2):
        left, right = [], []
        for step in range(pair, tables[0].shape[0], 2):
            high, low, row, target = (table[step, index : index + 1, :] for table in tables)
            left.append(jnp.concatenate([value_at(narrow, row, high), value_at(narrow, row, low)], axis=0))
            right.append(ones_at(wide, target))
        total = dot_t(jnp.concatenate(left, axis=1), jnp.concatenate(right, axis=1))
        pairs.append(total[:SPAN] + total[SPAN:])
    return jnp.concatenate(pairs, axis=1)


def decode_kernel(groups, lists, out, *tables):
    prepare(lists, groups, tables)
    narrow, wide = counter(SPAN), counter(2 * SPAN)
    for index in range(groups):
        out[index * SPAN : (index + 1) * SPAN, :] = decode_group(index, narrow, wide, tables)


def decode_last_kernel(groups, lists, held, out, squares, *tables):
    prepare(lists, groups, tables)
    narrow, wide = counter(SPAN), counter(2 * SPAN)
    squared = jnp.zeros((8, WIDE), F32)
    for index in range(groups):
        rows = slice(index * SPAN, (index + 1) * SPAN)
        total = held[rows, :] + decode_group(index, narrow, wide, tables)
        out[rows, :] = total
        squared = squared + jnp.sum((total * total).reshape(8, 8, WIDE), axis=0)
    squares[...] = squared[:, :128] + squared[:, 128:]


def update_kernel(total, tables, out, high, low, stack):
    groups = total.shape[0] // SPAN
    for index in range(groups):
        rows = slice(index * SPAN, (index + 1) * SPAN)
        high[rows, :], low[rows, :] = split(total[rows, :])
    out[...] = inverse(high, low, tables, stack, groups)


def apply_kernel(entries, chunks, weights, update, squares, out, buf, sems):
    total = jnp.sum(jnp.sum(squares[...], axis=0, keepdims=True), axis=1, keepdims=True)
    scale = lax.rsqrt(total / entries + 1.0)
    step = update.shape[0] // chunks
    copies = []
    for at in range(chunks):
        rows = pl.ds(at * step, step)
        buf[rows, :] = weights[rows, :] - update[rows, :] * scale
        copies.append(pltpu.make_async_copy(buf.at[rows, :], out.at[rows, :], sems.at[at]))
        copies[-1].start()
    for copy in copies:
        copy.wait()


def call(kernel, shapes, flops, *args, spaces=None, scratch=(), space=pltpu.VMEM):
    spaces = spaces or {}
    specs = [pl.BlockSpec(memory_space=spaces.get(at, pltpu.VMEM)) for at in range(len(args))]
    out_specs = jax.tree.map(lambda _: pl.BlockSpec(memory_space=space), shapes)
    return pl.pallas_call(
        kernel,
        out_shape=shapes,
        in_specs=specs,
        out_specs=out_specs,
        scratch_shapes=list(scratch),
        cost_estimate=pl.CostEstimate(flops=flops, bytes_accessed=1 << 20, transcendentals=0),
        compiler_params=pltpu.CompilerParams(vmem_limit_bytes=VMEM_LIMIT),
    )(*args)


def local(replicas, parts, gradient, momentum, weights, positions):
    table = dct_table()
    columns = jnp.asarray(np.concatenate(halves(table.T), axis=0))
    backward = jnp.asarray(operands(table.T))
    height, width = weights.shape
    groups = width // WIDE
    spans, kept = positions.shape[2:]
    chunks = 1
    field = jax.ShapeDtypeStruct((height, width), F32)
    tall = jax.ShapeDtypeStruct((groups * SPAN, WIDE), F32)
    half = pltpu.VMEM((groups * SPAN, WIDE), BF16)
    stack = pltpu.VMEM((3 * SPAN, width), BF16)
    message, summed, sides, column = call(
        functools.partial(pick_kernel, chunks),
        (
            jax.ShapeDtypeStruct((1, 32, 128), F32),
            field,
            jax.ShapeDtypeStruct((groups, WIDE, 2 * 128), BF16),
            jax.ShapeDtypeStruct((groups, SPAN, 128), F32),
        ),
        1 << 30,
        pltpu.with_memory_space_constraint(gradient, pltpu.HBM),
        pltpu.with_memory_space_constraint(momentum, pltpu.HBM),
        pltpu.with_memory_space_constraint(jnp.swapaxes(positions[0, 0], 0, 1), pltpu.HBM),
        pltpu.with_memory_space_constraint(columns, pltpu.HBM),
        spaces={0: pltpu.HBM, 1: pltpu.HBM, 2: pltpu.HBM, 3: pltpu.HBM},
        scratch=(
            pltpu.VMEM((height, width), BF16),
            pltpu.VMEM((height, width), F32),
            pltpu.VMEM((kept, spans), jnp.int32),
            pltpu.VMEM(columns.shape, BF16),
            pltpu.VMEM((spans, kept), jnp.int32),
            pltpu.VMEM((SPAN, width), BF16),
            pltpu.SemaphoreType.DMA((2 * chunks + 2,)),
        ),
    )
    new_momentum = call(
        momentum_kernel,
        jax.ShapeDtypeStruct(momentum.shape, F32),
        1 << 31,
        message,
        summed,
        sides,
        column,
        space=pltpu.HBM,
        scratch=(pltpu.VMEM((height, width), F32), pltpu.SemaphoreType.DMA((groups,))),
    )
    held = message
    bit = 1
    fillers = [new_momentum]
    while 2 * bit < replicas:
        other = lax.ppermute(held, "dp", [(at, at ^ bit) for at in range(replicas)])
        held = jnp.concatenate([held, other], axis=0)
        if fillers:
            held, _ = lax.optimization_barrier((held, fillers.pop(0)))
        bit *= 2
    other = lax.ppermute(held, "dp", [(at, at ^ bit) for at in range(replicas)])
    tables = tuple(pltpu.VMEM((bit, groups, 128), F32) for _ in range(4))
    own_total = call(
        functools.partial(decode_kernel, groups),
        tall,
        1 << 30,
        held,
        scratch=tables,
    )
    total, squares = call(
        functools.partial(decode_last_kernel, groups),
        (tall, jax.ShapeDtypeStruct((8, 128), F32)),
        1 << 30,
        other,
        own_total,
        scratch=tables,
    )
    update = call(update_kernel, field, 1 << 31, total, backward, scratch=(half, half, stack))
    step = 1
    while step < parts:
        flip = 2 * step - 1
        squares = squares + lax.ppermute(squares, "mp", [(at, at ^ flip) for at in range(parts)])
        step *= 2
    new_weights = call(
        functools.partial(apply_kernel, float(height * width * parts), 4),
        field,
        1 << 20,
        weights,
        update,
        squares,
        space=pltpu.HBM,
        scratch=(pltpu.VMEM((height, width), F32), pltpu.SemaphoreType.DMA((4,))),
    )
    return new_momentum, new_weights


def solution(mesh):
    placed = (P("dp", None, "mp"), P("dp", None, "mp"), P(None, "mp"), P("dp", None, "mp", None))
    return jax.shard_map(
        functools.partial(local, mesh.shape["dp"], mesh.shape["mp"]),
        mesh=mesh,
        in_specs=placed,
        out_specs=(P("dp", None, "mp"), P(None, "mp")),
        check_vma=False,
    )
```

```python
import functools

import jax
import jax.numpy as jnp
import numpy as np
from jax import lax
from jax.experimental import pallas as pl
from jax.experimental.pallas import tpu as pltpu
from jax.sharding import PartitionSpec as P

SPAN = 64
QUAD = 4
WIDE = SPAN * QUAD
SHIFT = 6
F32 = jnp.float32
BF16 = jnp.bfloat16
VMEM_LIMIT = 24 * 1024 * 1024


def dct_table():
    column = np.arange(SPAN, dtype=np.float64)
    factor = np.where(column == 0, np.sqrt(1.0 / SPAN), np.sqrt(2.0 / SPAN))
    angle = np.pi * (2.0 * column[None, :] + 1.0) * column[:, None] / (2.0 * SPAN)
    return (factor[:, None] * np.cos(angle)).astype(np.float32)


def halves(table):
    high = table.astype(BF16)
    return high, (table - high.astype(np.float32)).astype(BF16)


def operands(table):
    high, low = halves(table)
    rows = np.concatenate([high, high, low, np.zeros_like(low)], axis=1)
    blocks = halves(np.kron(np.eye(QUAD, dtype=np.float32), table.T))
    return np.concatenate([rows, *blocks], axis=0)


def split(value):
    high = value.astype(BF16)
    return high, (value - high.astype(F32)).astype(BF16)


def dot(left, right):
    return lax.dot_general(left, right, (((1,), (0,)), ((), ())), preferred_element_type=F32)


def dot_t(left, right):
    return lax.dot_general(left, right, (((1,), (1,)), ((), ())), preferred_element_type=F32)


def row_table(tables):
    return tables[:SPAN, : 3 * SPAN]


def along_lanes(high, low, tables):
    high_table = tables[SPAN : SPAN + WIDE, :]
    low_table = tables[SPAN + WIDE :, :]
    return dot(high, high_table) + dot(low, high_table) + dot(high, low_table)


def put_rows(stack, lanes, value):
    high, low = split(value)
    stack[:SPAN, lanes] = high
    stack[SPAN : 2 * SPAN, lanes] = low
    stack[2 * SPAN :, lanes] = high


def lane_target(place):
    quarter = lax.broadcasted_iota(jnp.int32, place.shape, 1) // (128 // QUAD)
    return quarter * SPAN + (place & (SPAN - 1))


def counter(size):
    return lax.broadcasted_iota(jnp.int32, (size, 128), 0).astype(F32).astype(BF16).reshape(size // 16, 16, 128)


def same(count, wanted):
    row = jnp.broadcast_to(wanted, (16, wanted.shape[1])).astype(BF16)
    return count == row[None]


def ones_at(count, wanted):
    mask = same(count, wanted)
    return jnp.where(mask, jnp.ones((), BF16), jnp.zeros((), BF16)).reshape(-1, 128)


def value_at(count, wanted, value):
    row = jnp.broadcast_to(value, (16, 128)).astype(BF16)
    mask = same(count, wanted)
    return jnp.where(mask, jnp.broadcast_to(row[None], count.shape), jnp.zeros((), BF16)).reshape(-1, 128)


def pick_kernel(chunks, grad, mom, place, table, message, summed, sides, column, g_buf, m_buf, p_buf, t_buf, turned, hots, sems):
    width = summed.shape[1]
    groups = width // WIDE
    step = width // chunks
    copies = [
        pltpu.make_async_copy(place, p_buf, sems.at[2 * chunks]),
        pltpu.make_async_copy(table, t_buf, sems.at[2 * chunks + 1]),
    ]
    for at in range(chunks):
        lanes = pl.ds(at * step, step)
        copies.append(pltpu.make_async_copy(grad.at[0, :, lanes], g_buf.at[:, lanes], sems.at[2 * at]))
        copies.append(pltpu.make_async_copy(mom.at[0, :, lanes], m_buf.at[:, lanes], sems.at[2 * at + 1]))
    for copy in copies:
        copy.start()
    narrow = counter(SPAN)
    lane = lax.broadcasted_iota(jnp.int32, (16, 128), 1) // (128 // QUAD)
    masks = [jnp.where(lane == at, 1.0, 0.0).astype(BF16) == jnp.ones((), BF16) for at in range(QUAD)]
    message[...] = jnp.zeros_like(message)
    copies[0].wait()
    turned[...] = jnp.transpose(p_buf[...])
    places = jnp.concatenate([turned[pl.ds(at, groups, stride=QUAD), :] for at in range(QUAD)], axis=1)
    message[0, 16 : 16 + groups, :] = places.astype(F32)
    row_of = (places >> SHIFT).astype(F32)
    column_of = ((places & (SPAN - 1))).astype(F32)
    for index in range(groups):
        hots[:, index * WIDE : index * WIDE + 128] = ones_at(narrow, column_of[index : index + 1])
        hots[:, index * WIDE + 128 : (index + 1) * WIDE] = ones_at(narrow, row_of[index : index + 1])
    copies[1].wait()
    chosen = dot(t_buf[...], hots[...])
    for index in range(groups):
        at = index * WIDE
        for half in range(2):
            tall = slice(half * SPAN, (half + 1) * SPAN)
            piece = chosen[tall, at : at + 128].astype(BF16).reshape(SPAN // 16, 16, 128)
            for quarter in range(QUAD):
                kept = jnp.where(masks[quarter][None], piece, jnp.zeros((), BF16)).reshape(SPAN, 128)
                sides[index, quarter * SPAN : (quarter + 1) * SPAN, half * 128 : (half + 1) * 128] = kept
        column[index] = chosen[:SPAN, at + 128 : at + WIDE] + chosen[SPAN:, at + 128 : at + WIDE]
    for at in range(chunks):
        lanes = slice(at * step, (at + 1) * step)
        copies[2 + 2 * at].wait()
        copies[3 + 2 * at].wait()
        total = 0.9 * m_buf[:, lanes] + g_buf[:, lanes].astype(F32)
        summed[:, lanes] = total
        for index in range(at * step // WIDE, (at + 1) * step // WIDE):
            inner = index * WIDE - at * step
            high, low = split(total[:, inner : inner + WIDE])
            both = dot(jnp.concatenate([high, low], axis=0), sides[index])
            values = both[:SPAN, :128] + both[SPAN:, :128] + both[:SPAN, 128:]
            message[0, index : index + 1, :] = jnp.sum(values * column[index], axis=0, keepdims=True)


def inverse(high, low, tables, stack, groups):
    across = along_lanes(high[...], low[...], tables)
    for index in range(groups):
        lanes = slice(index * WIDE, (index + 1) * WIDE)
        put_rows(stack, lanes, across[index * SPAN : (index + 1) * SPAN, :])
    return dot(row_table(tables), stack[...])


def momentum_kernel(message, summed, sides, column, out, buf, sems):
    groups = column.shape[0]
    copies = []
    for index in range(groups):
        lanes = pl.ds(index * WIDE, WIDE)
        high, low = split(column[index] * message[0, index : index + 1, :])
        left = jnp.concatenate(
            [jnp.concatenate([high, high], axis=1), jnp.concatenate([low, jnp.zeros_like(low)], axis=1)], axis=0
        )
        both = dot_t(left, sides[index])
        buf[:, lanes] = summed[:, lanes] - (both[:SPAN] + both[SPAN:])
        copies.append(pltpu.make_async_copy(buf.at[:, lanes], out.at[0, :, lanes], sems.at[index]))
        copies[-1].start()
    for copy in copies:
        copy.wait()


def prepare(lists, groups, tables):
    order = lax.axis_index("dp") & (lists.shape[0] - 1)
    shape = (groups, 128)
    lane = lax.broadcasted_iota(jnp.int32, shape, 1)
    lower = lane < SPAN
    span = ((lane >> 5) & 1) * SPAN
    for step in range(0, lists.shape[0], 2):
        parts = []
        for which in (step ^ order, (step + 1) ^ order):
            value = lists[which, :groups, :]
            high = value.astype(BF16).astype(F32)
            places = lists[which, 16 : 16 + groups, :].astype(jnp.int32)
            target = span + (places & (SPAN - 1))
            parts.append((high, value - high, (places >> SHIFT).astype(F32), target.astype(F32)))
        for out, first, second in zip(tables, *parts):
            out[step] = jnp.where(lower, first, pltpu.roll(second, SPAN, 1))
            out[step + 1] = jnp.where(lower, pltpu.roll(first, SPAN, 1), second)


def decode_group(index, narrow, wide, tables):
    pairs = []
    for pair in range(2):
        left, right = [], []
        for step in range(pair, tables[0].shape[0], 2):
            high, low, row, target = (table[step, index : index + 1, :] for table in tables)
            left.append(jnp.concatenate([value_at(narrow, row, high), value_at(narrow, row, low)], axis=0))
            right.append(ones_at(wide, target))
        total = dot_t(jnp.concatenate(left, axis=1), jnp.concatenate(right, axis=1))
        pairs.append(total[:SPAN] + total[SPAN:])
    return jnp.concatenate(pairs, axis=1)


def decode_kernel(groups, lists, out, *tables):
    prepare(lists, groups, tables)
    narrow, wide = counter(SPAN), counter(2 * SPAN)
    for index in range(groups):
        out[index * SPAN : (index + 1) * SPAN, :] = decode_group(index, narrow, wide, tables)


def decode_last_kernel(groups, lists, held, out, squares, *tables):
    prepare(lists, groups, tables)
    narrow, wide = counter(SPAN), counter(2 * SPAN)
    squared = jnp.zeros((8, WIDE), F32)
    for index in range(groups):
        rows = slice(index * SPAN, (index + 1) * SPAN)
        total = held[rows, :] + decode_group(index, narrow, wide, tables)
        out[rows, :] = total
        squared = squared + jnp.sum((total * total).reshape(8, 8, WIDE), axis=0)
    squares[...] = squared[:, :128] + squared[:, 128:]


def update_kernel(total, tables, out, high, low, stack):
    groups = total.shape[0] // SPAN
    for index in range(groups):
        rows = slice(index * SPAN, (index + 1) * SPAN)
        high[rows, :], low[rows, :] = split(total[rows, :])
    out[...] = inverse(high, low, tables, stack, groups)


def apply_kernel(entries, chunks, weights, update, squares, out, buf, sems):
    total = jnp.sum(jnp.sum(squares[...], axis=0, keepdims=True), axis=1, keepdims=True)
    scale = lax.rsqrt(total / entries + 1.0)
    step = update.shape[0] // chunks
    copies = []
    for at in range(chunks):
        rows = pl.ds(at * step, step)
        buf[rows, :] = weights[rows, :] - update[rows, :] * scale
        copies.append(pltpu.make_async_copy(buf.at[rows, :], out.at[rows, :], sems.at[at]))
        copies[-1].start()
    for copy in copies:
        copy.wait()


def call(kernel, shapes, flops, *args, spaces=None, scratch=(), space=pltpu.VMEM):
    spaces = spaces or {}
    specs = [pl.BlockSpec(memory_space=spaces.get(at, pltpu.VMEM)) for at in range(len(args))]
    out_specs = jax.tree.map(lambda _: pl.BlockSpec(memory_space=space), shapes)
    return pl.pallas_call(
        kernel,
        out_shape=shapes,
        in_specs=specs,
        out_specs=out_specs,
        scratch_shapes=list(scratch),
        cost_estimate=pl.CostEstimate(flops=flops, bytes_accessed=1 << 20, transcendentals=0),
        compiler_params=pltpu.CompilerParams(vmem_limit_bytes=VMEM_LIMIT),
    )(*args)


def local(replicas, parts, gradient, momentum, weights, positions):
    table = dct_table()
    columns = jnp.asarray(np.concatenate(halves(table.T), axis=0))
    backward = jnp.asarray(operands(table.T))
    height, width = weights.shape
    groups = width // WIDE
    spans, kept = positions.shape[2:]
    chunks = 1
    field = jax.ShapeDtypeStruct((height, width), F32)
    tall = jax.ShapeDtypeStruct((groups * SPAN, WIDE), F32)
    half = pltpu.VMEM((groups * SPAN, WIDE), BF16)
    stack = pltpu.VMEM((3 * SPAN, width), BF16)
    message, summed, sides, column = call(
        functools.partial(pick_kernel, chunks),
        (
            jax.ShapeDtypeStruct((1, 32, 128), F32),
            field,
            jax.ShapeDtypeStruct((groups, WIDE, 2 * 128), BF16),
            jax.ShapeDtypeStruct((groups, SPAN, 128), F32),
        ),
        1 << 30,
        pltpu.with_memory_space_constraint(gradient, pltpu.HBM),
        pltpu.with_memory_space_constraint(momentum, pltpu.HBM),
        pltpu.with_memory_space_constraint(jnp.swapaxes(positions[0, 0], 0, 1), pltpu.HBM),
        pltpu.with_memory_space_constraint(columns, pltpu.HBM),
        spaces={0: pltpu.HBM, 1: pltpu.HBM, 2: pltpu.HBM, 3: pltpu.HBM},
        scratch=(
            pltpu.VMEM((height, width), BF16),
            pltpu.VMEM((height, width), F32),
            pltpu.VMEM((kept, spans), jnp.int32),
            pltpu.VMEM(columns.shape, BF16),
            pltpu.VMEM((spans, kept), jnp.int32),
            pltpu.VMEM((SPAN, width), BF16),
            pltpu.SemaphoreType.DMA((2 * chunks + 2,)),
        ),
    )
    new_momentum = call(
        momentum_kernel,
        jax.ShapeDtypeStruct(momentum.shape, F32),
        1 << 31,
        message,
        summed,
        sides,
        column,
        space=pltpu.HBM,
        scratch=(pltpu.VMEM((height, width), F32), pltpu.SemaphoreType.DMA((groups,))),
    )
    held = message
    bit = 1
    fillers = [new_momentum]
    while 2 * bit < replicas:
        other = lax.ppermute(held, "dp", [(at, at ^ bit) for at in range(replicas)])
        held = jnp.concatenate([held, other], axis=0)
        if fillers:
            held, _ = lax.optimization_barrier((held, fillers.pop(0)))
        bit *= 2
    other = lax.ppermute(held, "dp", [(at, at ^ bit) for at in range(replicas)])
    tables = tuple(pltpu.VMEM((bit, groups, 128), F32) for _ in range(4))
    own_total = call(
        functools.partial(decode_kernel, groups),
        tall,
        1 << 30,
        held,
        scratch=tables,
    )
    total, squares = call(
        functools.partial(decode_last_kernel, groups),
        (tall, jax.ShapeDtypeStruct((8, 128), F32)),
        1 << 30,
        other,
        own_total,
        scratch=tables,
    )
    update = call(update_kernel, field, 1 << 31, total, backward, scratch=(half, half, stack))
    for step in reversed(range(1, parts.bit_length())):
        flip = 2**step - 1
        squares = squares + lax.ppermute(squares, "mp", [(at, at ^ flip) for at in range(parts)])
        squares, update = lax.optimization_barrier((squares, update))
    new_weights = call(
        functools.partial(apply_kernel, float(height * width * parts), 4),
        field,
        1 << 20,
        weights,
        update,
        squares,
        space=pltpu.HBM,
        scratch=(pltpu.VMEM((height, width), F32), pltpu.SemaphoreType.DMA((4,))),
    )
    return new_momentum, new_weights


def solution(mesh):
    placed = (P("dp", None, "mp"), P("dp", None, "mp"), P(None, "mp"), P("dp", None, "mp", None))
    return jax.shard_map(
        functools.partial(local, mesh.shape["dp"], mesh.shape["mp"]),
        mesh=mesh,
        in_specs=placed,
        out_specs=(P("dp", None, "mp"), P(None, "mp")),
        check_vma=False,
    )
```
